32 devices in a mesh: groups: 2 (over y), tok: 4 (over z), lat: 2 (over x), rep: 2 (over core).
Axes of the slice: x: 2, y: 2, z: 4, core: 2. Of those that a mesh axis runs over, the one named last changes fastest.
Arguments:
- tokens: bfloat16 [2048, 512], P(('groups', 'tok', 'lat')), parts along dimension 0, may hold values from -15 to 15
- latents: bfloat16 [768, 512], P(('tok', 'lat')), may hold values from -6 to 6
- w_tok: bfloat16 [1, 512, 2, 512], P(None, None, None, 'rep'), may hold values from -1.5 to 1.5
- w_lat: bfloat16 [1, 512, 2, 512], P(None, None, None, 'rep'), may hold values from -1.5 to 1.5
- o_tok: bfloat16 [1, 512, 512], P(None, 'rep'), may hold values from -0.25 to 0.25
- o_lat: bfloat16 [1, 512, 512], P(None, 'rep'), may hold values from -0.25 to 0.25
- g_tok: float32 [1, 512], replicated, may hold values from 0.1 to 1.9
- g_lat: float32 [1, 512], replicated, may hold values from 0.1 to 1.9
Outputs:
- tokens_out: bfloat16 [2048, 512], P(('groups', 'tok', 'lat')), parts along dimension 0
- latents_out: bfloat16 [1536, 512], P(('groups', 'tok', 'lat')), parts along dimension 0
The draws below stay inside these ranges and needn't reach their ends.
There are 2 independent parts, one for each index of `groups`. The reference program is written for one: setup_inputs(seed, part) draws one part's arguments, and reference() takes and returns one part's arrays. A program takes and returns all parts, laid end to end along the dimension named above; an argument that names none is the same for every part. Nothing has to cross between parts.
All inputs are finite; a program needn't handle non-finite values.
Results may differ from the reference program's by a relative error of at most 0.0068.
Values may be sent and summed in bfloat16 or wider, within the bound.
A program may use at most 64 MiB of HBM per device.

```python
import jax
import jax.numpy as jnp
from jax import lax

D = 512
HEADS = 8
NLAT = 768
LAYERS = 1
TOK_DEV = 128
NTOK = 1024


def projection_draw(key, salt):
    base = jax.random.normal(jax.random.fold_in(key, salt), (LAYERS, D, 2, D), jnp.float32)
    base = jnp.clip(base, -6.0, 6.0) / jnp.sqrt(jnp.float32(D))
    base = jnp.clip(base, -1.5, 1.5)
    return base.astype(jnp.bfloat16)


def draw_w_tok(key, part):
    return projection_draw(key, 21)


def draw_w_lat(key, part):
    return projection_draw(key, 22)


def draw_tokens(key, part):
    noise = jnp.clip(jax.random.normal(jax.random.fold_in(key, 31), (NTOK, D), jnp.float32), -6.0, 6.0)
    values = noise
    return values.astype(jnp.bfloat16)


def levels(rng, extent, shards, least, largest):
    def one(dim, shards_of):
        steps = jax.random.uniform(jax.random.fold_in(jax.random.fold_in(rng, 6), dim), (shards_of,), jnp.float32, least / len(shards), largest / len(shards))
        return jnp.repeat(jnp.exp(steps), extent[dim] // shards_of).reshape((-1,) + (1,) * (len(extent) - dim - 1))

    gain = one(*shards[0])
    for cut in shards[1:]:
        gain = gain * one(*cut)
    return gain


def centred(rng, extent, width, limit, split=(), held_as=jnp.bfloat16):
    values = jax.random.normal(rng, extent, jnp.float32) * width
    if len(split) > 0:
        values = levels(rng, extent, split, -0.22, 0.18) * values
    return jnp.clip(values, min=-limit, max=limit).astype(held_as)


def setup_inputs(seed: int = 0, part: int = 0) -> dict:
    key_of = jax.random.split(jax.random.key(seed), 9)
    part_keys = jax.random.split(jax.random.fold_in(key_of[8], part), 9)
    tokens = draw_tokens(jax.random.fold_in(jax.random.fold_in(key_of[8], part), 71), part)
    latents = centred(key_of[1], (NLAT, D), 1.0, 6.0, ((0, 8),))
    w_tok = draw_w_tok(jax.random.fold_in(key_of[8], 71), part)
    w_lat = draw_w_lat(jax.random.fold_in(key_of[8], 71), part)
    o_tok = centred(key_of[4], (LAYERS, D, D), D ** -0.5, 0.25, ((1, 2),))
    o_lat = centred(key_of[5], (LAYERS, D, D), D ** -0.5, 0.25, ((1, 2),))
    g_tok = jnp.clip(1.0 + 0.18 * jax.random.normal(key_of[6], (LAYERS, D), jnp.float32), 0.1, 1.9)
    g_lat = jnp.clip(1.0 + 0.18 * jax.random.normal(key_of[7], (LAYERS, D), jnp.float32), 0.1, 1.9)
    return {"tokens": tokens, "latents": latents, "w_tok": w_tok, "w_lat": w_lat, "o_tok": o_tok, "o_lat": o_lat, "g_tok": g_tok, "g_lat": g_lat}


EPS = 1e-06

def rms_scale(source, gain_row):
    widened = source.astype(jnp.float32)
    mean_sq = lax.optimization_barrier(jnp.mean(widened * widened, axis=-1, keepdims=True))
    return (widened * lax.rsqrt(mean_sq + EPS) * gain_row).astype(jnp.bfloat16)

def reference(tokens, latents, w_tok, w_lat, o_tok, o_lat, g_tok, g_lat):
    head_size = D // HEADS
    scale = head_size ** (-0.5)
    block_count = NTOK // TOK_DEV
    for layer_index in range(LAYERS):
        tok_in = rms_scale(tokens, g_tok[layer_index])
        lat_in = rms_scale(latents, g_lat[layer_index])
        tok_proj = jnp.dot(tok_in, w_tok[layer_index].reshape(D, 2 * D), preferred_element_type=jnp.float32)
        tok_proj = tok_proj.astype(jnp.bfloat16).reshape(NTOK, 2, HEADS, head_size)
        lat_proj = jnp.dot(lat_in, w_lat[layer_index].reshape(D, 2 * D), preferred_element_type=jnp.float32)
        lat_proj = lat_proj.astype(jnp.bfloat16).reshape(NLAT, 2, HEADS, head_size)
        lat_key = lat_proj[:, 0].astype(jnp.float32)
        lat_val = lat_proj[:, 1].astype(jnp.float32)

        def one_block(block_index):
            block_rows = lax.dynamic_slice_in_dim(tok_proj, (block_index * TOK_DEV).astype(jnp.int32), TOK_DEV, 0)
            tok_key = block_rows[:, 0].astype(jnp.float32)
            tok_val = block_rows[:, 1].astype(jnp.float32)
            scores = jnp.einsum('lhd,thd->hlt', lat_key, tok_key) * scale
            peak_tok = lax.optimization_barrier(jnp.max(scores, axis=1, keepdims=True))
            tok_exp = jnp.exp(scores - peak_tok)
            tok_weights = lax.optimization_barrier((tok_exp / lax.optimization_barrier(jnp.sum(tok_exp, axis=1, keepdims=True))).astype(jnp.bfloat16))
            tok_att = jnp.einsum('hlt,lhd->thd', tok_weights.astype(jnp.float32), lat_val).astype(jnp.bfloat16)
            peak_lat = lax.optimization_barrier(jnp.max(scores, axis=2))
            lat_exp = jnp.exp(scores - peak_lat[:, :, None])
            block_den = lax.optimization_barrier(jnp.sum(lat_exp, axis=2))
            lat_round = lax.optimization_barrier(lat_exp.astype(jnp.bfloat16))
            block_num = jnp.einsum('hlt,thd->lhd', lat_round.astype(jnp.float32), tok_val)
            return (tok_att, block_num, block_den, peak_lat)
        tok_att, block_num, block_den, peaks = lax.map(one_block, jnp.arange(block_count, dtype=jnp.int32))
        score_top = lax.optimization_barrier(jnp.max(peaks, axis=0))
        factor = jnp.exp(peaks - score_top)
        num_total = jnp.einsum('bhl,blhd->lhd', factor, block_num)
        den_total = lax.optimization_barrier(jnp.sum(factor * block_den, axis=0))
        lat_att = (num_total / jnp.transpose(den_total)[:, :, None]).astype(jnp.bfloat16).reshape(NLAT, D)
        tok_att = tok_att.reshape(NTOK, D)
        tok_sum = jnp.dot(tok_att, o_tok[layer_index], preferred_element_type=jnp.float32)
        lat_sum = jnp.dot(lat_att, o_lat[layer_index], preferred_element_type=jnp.float32)
        tokens = (tokens.astype(jnp.float32) + tok_sum).astype(jnp.bfloat16)
        latents = (latents.astype(jnp.float32) + lat_sum).astype(jnp.bfloat16)
    return (tokens, latents)
```

```python
import functools

import jax
import jax.numpy as jnp
from jax import lax
from jax.experimental import pallas as pl
from jax.experimental.pallas import tpu as pltpu
from jax.sharding import PartitionSpec as P

D = 512
HEADS = 8


EPS = 1e-06


def rms_scale(source, gain_row):
    widened = source.astype(jnp.float32)
    mean_sq = jnp.mean(widened * widened, axis=-1, keepdims=True)
    return (widened * lax.rsqrt(mean_sq + EPS) * gain_row).astype(jnp.bfloat16)


def head_terms(per_head):
    tok_key, tok_val, lat_key, lat_val = per_head
    scale = lat_key.shape[1] ** (-0.5)
    scores = (
        lax.dot_general(
            lat_key, tok_key, (((1,), (1,)), ((), ())), preferred_element_type=jnp.float32
        )
        * scale
    )
    peak_tok = jnp.max(scores, axis=0, keepdims=True)
    tok_exp = jnp.exp(scores - peak_tok)
    tok_weights = (tok_exp / jnp.sum(tok_exp, axis=0, keepdims=True)).astype(jnp.bfloat16)
    tok_att = lax.dot_general(
        tok_weights, lat_val, (((0,), (0,)), ((), ())), preferred_element_type=jnp.float32
    )
    peak_lat = jnp.max(scores, axis=1)
    lat_exp = jnp.exp(scores - peak_lat[:, None])
    block_den = jnp.sum(lat_exp, axis=1)
    block_num = jnp.dot(lat_exp.astype(jnp.bfloat16), tok_val, preferred_element_type=jnp.float32)
    return (tok_att.astype(jnp.bfloat16), block_num, block_den, peak_lat)


def body(tokens, latents, w_tok, w_lat, o_tok, o_lat, g_tok, g_lat):
    head_size = D // HEADS
    row_count = tokens.shape[0]
    model_width = tokens.shape[1]
    half_width = w_tok.shape[3]
    head_count = half_width // head_size
    tok_in = rms_scale(tokens, g_tok[0])
    lat_in = rms_scale(latents, g_lat[0])
    tok_proj = jnp.dot(
        tok_in, w_tok[0].reshape(model_width, 2 * half_width), preferred_element_type=jnp.float32
    )
    tok_proj = tok_proj.astype(jnp.bfloat16).reshape(row_count, 2, head_count, head_size)
    lat_own = jnp.dot(
        lat_in, w_lat[0].reshape(model_width, 2 * half_width), preferred_element_type=jnp.float32
    )
    lat_own = lat_own.astype(jnp.bfloat16).reshape(-1, 2, half_width)
    lat_proj = lax.all_gather(lat_own, ("tok", "lat"), axis=0, tiled=True)
    lat_count = lat_proj.shape[0]
    lat_proj = lat_proj.reshape(lat_count, 2, head_count, head_size)
    per_head = (
        jnp.transpose(tok_proj[:, 0], (1, 0, 2)),
        jnp.transpose(tok_proj[:, 1], (1, 0, 2)),
        jnp.transpose(lat_proj[:, 0], (1, 0, 2)),
        jnp.transpose(lat_proj[:, 1], (1, 0, 2)),
    )
    tok_att, block_num, block_den, peaks = lax.map(head_terms, per_head)
    tok_att = jnp.transpose(tok_att, (1, 0, 2)).reshape(row_count, half_width)
    block_num = jnp.transpose(block_num, (1, 0, 2))
    block_den = jnp.transpose(block_den)
    peaks = jnp.transpose(peaks)
    got_num = lax.all_to_all(
        block_num.reshape(lat_count, half_width),
        ("tok", "lat"),
        split_axis=0,
        concat_axis=0,
        tiled=True,
    )
    got_den = lax.all_to_all(block_den, ("tok", "lat"), split_axis=0, concat_axis=0, tiled=True)
    got_peak = lax.all_to_all(peaks, ("tok", "lat"), split_axis=0, concat_axis=0, tiled=True)
    sources = lax.axis_size(("tok", "lat"))
    got_num = got_num.reshape(sources, -1, head_count, head_size)
    got_den = got_den.reshape(sources, -1, head_count)
    got_peak = got_peak.reshape(sources, -1, head_count)
    score_top = jnp.max(got_peak, axis=0)
    factor = jnp.exp(got_peak - score_top)
    num_own = jnp.sum(got_num * factor[:, :, :, None], axis=0)
    den_own = jnp.sum(got_den * factor, axis=0)
    lat_att = (num_own / den_own[:, :, None]).astype(jnp.bfloat16).reshape(-1, half_width)
    lat_part = jnp.dot(lat_att, o_lat[0], preferred_element_type=jnp.float32)
    lat_sum = lax.psum(lat_part, "rep")
    latents = (latents.astype(jnp.float32) + lat_sum).astype(jnp.bfloat16)
    tok_part = jnp.dot(tok_att, o_tok[0], preferred_element_type=jnp.float32)
    tok_sum = lax.psum(tok_part, "rep")
    tokens = (tokens.astype(jnp.float32) + tok_sum).astype(jnp.bfloat16)
    return (tokens, latents)

MESH_ID = pl.DeviceIdType.MESH
UP, DOWN, ACROSS, PARTNER = 0, 1, 2, 3
LANES = 128
VMEM_BYTES = 67_043_328


def arrival_order(depth, z):
    found = []
    for row in range(depth):
        far = abs(row - z)
        if far:
            found.append((far, 0, -row, row, 0))
        found.append((far + 1, 1, -row, row, 1))
    found.sort()
    return [(row, across) for *_, row, across in found]


def looked_up(table, z, n):
    total = 0
    for i, entries in enumerate(table):
        for j, entry in enumerate(entries):
            if entry:
                total = total + entry * ((z == i) & (n == j)).astype(jnp.int32)
    return total


def kernel(
    depth,
    wide,
    tok_hbm,
    lat_hbm,
    w_tok_hbm,
    w_lat_hbm,
    o_tok_hbm,
    o_lat_hbm,
    g_tok_hbm,
    g_lat_hbm,
    tok_out,
    lat_out,
    tok_all,
    lat_all,
    tok_own,
    lat_own,
    gain_ref,
    w_raw,
    w_ref,
    o_ref,
    query,
    peak,
    total,
    mixed,
    tok_att,
    lat_att,
    send_sem,
    recv_sem,
    load_sem,
    o_send,
    o_recv,
    att_send,
    att_recv,
):
    z = lax.axis_index("tok")
    x = lax.axis_index("lat")
    core = lax.axis_index("rep")
    across = 1 - x
    width = tok_all.shape[1]
    sizes = (lat_own.shape[0], tok_own.shape[0])
    half_width = w_raw.shape[3]
    head_size = D // HEADS
    pairs = half_width // LANES
    blocks = depth * wide
    me = z * wide + x
    bf16, f32 = jnp.bfloat16, jnp.float32
    devices = {
        UP: {"tok": z + 1},
        DOWN: {"tok": z - 1},
        ACROSS: {"lat": across},
        PARTNER: {"rep": 1 - core},
    }
    has_up = z + 1 < depth
    has_down = z > 0
    barrier = pltpu.get_barrier_semaphore()

    def greet(way):
        pl.semaphore_signal(barrier, inc=1, device_id=devices[way], device_id_type=MESH_ID)

    pl.when(has_down)(lambda: greet(DOWN))
    pl.when(has_up)(lambda: greet(UP))
    greet(ACROSS)
    greet(PARTNER)

    own = (lat_own, tok_own)
    gathered = (lat_all, tok_all)
    mine = pl.ds(pl.multiple_of(core * half_width, LANES), half_width)
    loads = [
        pltpu.make_async_copy(lat_hbm, lat_own, load_sem.at[0]),
        pltpu.make_async_copy(tok_hbm, tok_own, load_sem.at[1]),
        pltpu.make_async_copy(g_lat_hbm, gain_ref.at[0], load_sem.at[2]),
        pltpu.make_async_copy(g_tok_hbm, gain_ref.at[1], load_sem.at[3]),
        pltpu.make_async_copy(w_lat_hbm.at[0], w_raw.at[0], load_sem.at[4]),
        pltpu.make_async_copy(w_tok_hbm.at[0], w_raw.at[1], load_sem.at[5]),
        pltpu.make_async_copy(o_lat_hbm.at[0], o_ref.at[0, mine], load_sem.at[6]),
        pltpu.make_async_copy(o_tok_hbm.at[0], o_ref.at[1, mine], load_sem.at[7]),
    ]
    for load in loads:
        load.start()

    def block_rows(kind, block):
        return pl.ds(pl.multiple_of(block * sizes[kind], 16), sizes[kind])

    for kind in range(2):
        loads[kind].wait()
        loads[2 + kind].wait()
        gathered[kind][block_rows(kind, me), :] = rms_scale(own[kind][...], gain_ref[kind])

    pl.semaphore_wait(barrier, 2 + has_up.astype(jnp.int32) + has_down.astype(jnp.int32))

    def part(kind, block, half):
        rows = sizes[kind] // 2
        start = pl.multiple_of(block * sizes[kind] + half * rows, 16)
        return gathered[kind].at[pl.ds(start, rows)]

    def piece(kind, block, way):
        target = part(kind, block, core)
        return pltpu.make_async_remote_copy(
            src_ref=target,
            dst_ref=target,
            send_sem=send_sem.at[way, kind, block],
            recv_sem=recv_sem.at[core, kind, block],
            device_id=devices[way],
            device_id_type=MESH_ID,
        )

    def landed(kind, block, half):
        target = part(kind, block, half)
        pltpu.make_async_copy(target, target, recv_sem.at[half, kind, block]).wait()

    def own_ways(act):
        pl.when(has_down)(lambda: act(DOWN))
        pl.when(has_up)(lambda: act(UP))
        act(ACROSS)

    orders = [arrival_order(depth, row) for row in range(depth)]
    rows_table = [[row for row, _ in order] for order in orders]
    across_table = [[flag for _, flag in order] for order in orders]

    def arrival(n):
        row = looked_up(rows_table, z, n)
        crossed = looked_up(across_table, z, n)
        column = x + crossed * (across - x)
        return row, crossed, row * wide + column

    def relay_ways(row, crossed, act):
        straight = crossed == 0
        pl.when(straight & (row > z) & has_down)(lambda: act(DOWN))
        pl.when(straight & (row < z) & has_up)(lambda: act(UP))
        pl.when(straight)(lambda: act(ACROSS))
        act(PARTNER)

    def relay(n):
        row, crossed, block = arrival(n)
        for kind in range(2):
            landed(kind, block, core)
            relay_ways(row, crossed, lambda way: piece(kind, block, way).start())

    for kind in range(2):
        own_ways(lambda way: piece(kind, me, way).start())

    o_copies = [
        pltpu.make_async_remote_copy(
            src_ref=hbm.at[0],
            dst_ref=o_ref.at[i, mine],
            send_sem=o_send.at[i],
            recv_sem=o_recv.at[i],
            device_id=devices[PARTNER],
            device_id_type=MESH_ID,
        )
        for i, hbm in enumerate((o_lat_hbm, o_tok_hbm))
    ]
    for copy in o_copies:
        copy.start()

    def project(kind, block):
        both = jnp.dot(
            gathered[kind][block_rows(kind, block), :],
            w_ref[kind],
            preferred_element_type=f32,
        ).astype(bf16)
        return both[:, :half_width], both[:, half_width:]

    def attend(kind, key, value, first):
        for pair in range(pairs):
            lanes = slice(pair * LANES, (pair + 1) * LANES)
            scores = lax.dot_general(
                key[:, lanes],
                query[kind, pair],
                (((1,), (1,)), ((), ())),
                preferred_element_type=f32,
            )
            top = jnp.max(scores, axis=0, keepdims=True)
            if not first:
                old = peak[kind, pair]
                top = jnp.maximum(old, top)
            weights = jnp.exp(scores - top)
            added = jnp.sum(weights, axis=0, keepdims=True)
            product = lax.dot_general(
                value[:, lanes],
                weights.astype(bf16),
                (((0,), (0,)), ((), ())),
                preferred_element_type=f32,
            )
            span = product.shape[1] // 2
            upper = product[:head_size, :span]
            lower = product[head_size:, span:]
            base = pair * LANES
            if first:
                total[kind, pair] = added
                mixed[kind, base : base + head_size] = upper
                mixed[kind, base + head_size : base + LANES] = lower
            else:
                shrink = jnp.exp(old - top)
                total[kind, pair] = total[kind, pair] * shrink + added
                mixed[kind, base : base + head_size] = (
                    mixed[kind, base : base + head_size] * shrink[:, :span] + upper
                )
                mixed[kind, base + head_size : base + LANES] = (
                    mixed[kind, base + head_size : base + LANES] * shrink[:, span:] + lower
                )
            peak[kind, pair] = top

    for kind in range(2):
        loads[4 + kind].wait()
        w_ref[kind] = w_raw[kind].reshape(width, 2 * half_width)

    kept = []
    span = query.shape[2] // 2
    query[...] = jnp.zeros_like(query)
    for kind in range(2):
        key, value = project(kind, me)
        kept.append((key, value))
        scaled = key * jnp.asarray(head_size ** (-0.5), bf16)
        for pair in range(pairs):
            part_key = scaled[:, pair * LANES : (pair + 1) * LANES]
            leading = lax.broadcasted_iota(jnp.int32, part_key.shape, 1) < head_size
            zero = jnp.zeros_like(part_key)
            query[kind, pair, : sizes[kind]] = jnp.where(leading, part_key, zero)
            query[kind, pair, span : span + sizes[kind]] = jnp.where(leading, zero, part_key)
    for kind in range(2):
        attend(kind, *kept[1 - kind], True)

    def process(n):
        _, _, block = arrival(n)
        both = []
        for kind in range(2):
            landed(kind, block, 1 - core)
            both.append(project(kind, block))
        for kind in range(2):
            attend(kind, *both[1 - kind], False)

    def step(n, carry):
        pl.when(n < blocks - 1)(lambda: relay(n))
        pl.when(n > 0)(lambda: process(n - 1))
        return carry

    lax.fori_loop(0, blocks, step, 0)

    attended = (lat_att, tok_att)
    att_copies = []
    for kind in range(2):
        for pair in range(pairs):
            scale = 1.0 / total[kind, pair]
            base = pair * LANES
            attended[kind][core, base : base + head_size] = (
                mixed[kind, base : base + head_size] * scale[:, :span]
            ).astype(bf16)
            attended[kind][core, base + head_size : base + LANES] = (
                mixed[kind, base + head_size : base + LANES] * scale[:, span:]
            ).astype(bf16)
        copy = pltpu.make_async_remote_copy(
            src_ref=attended[kind].at[core],
            dst_ref=attended[kind].at[core],
            send_sem=att_send.at[kind],
            recv_sem=att_recv.at[kind],
            device_id=devices[PARTNER],
            device_id_type=MESH_ID,
        )
        copy.start()
        att_copies.append(copy)

    def mapped(kind, half):
        rows = pl.ds(pl.multiple_of(half * half_width, LANES), half_width)
        return lax.dot_general(
            attended[kind][half],
            o_ref[kind, rows, :],
            (((0,), (0,)), ((), ())),
            preferred_element_type=f32,
        )[: sizes[kind]]

    outs = (lat_out, tok_out)
    sums = []
    for kind in range(2):
        loads[6 + kind].wait()
        sums.append(own[kind][...].astype(f32) + mapped(kind, core))
    for kind in range(2):
        o_copies[kind].wait()
        att_copies[kind].wait()
        outs[kind][...] = (sums[kind] + mapped(kind, 1 - core)).astype(bf16)

    for kind in range(2):
        own_ways(lambda way: piece(kind, me, way).wait_send())

    def drain(n, carry):
        row, crossed, block = arrival(n)
        for kind in range(2):
            relay_ways(row, crossed, lambda way: piece(kind, block, way).wait_send())
        return carry

    lax.fori_loop(0, blocks - 1, drain, 0)


def gathered_body(tokens, latents, w_tok, w_lat, o_tok, o_lat, g_tok, g_lat):
    depth = lax.axis_size("tok")
    wide = lax.axis_size("lat")
    tok_rows, width = tokens.shape
    lat_rows = latents.shape[0]
    half_width = w_tok.shape[3]
    blocks = depth * wide
    pairs = half_width // LANES
    span = -(-max(tok_rows, lat_rows) // LANES) * LANES
    bf16, f32 = jnp.bfloat16, jnp.float32
    vmem = pl.BlockSpec(memory_space=pltpu.VMEM)
    hbm = pl.BlockSpec(memory_space=pltpu.MemorySpace.HBM)
    dma = pltpu.SemaphoreType.DMA
    return pl.pallas_call(
        functools.partial(kernel, depth, wide),
        out_shape=(
            jax.ShapeDtypeStruct(tokens.shape, bf16),
            jax.ShapeDtypeStruct(latents.shape, bf16),
        ),
        in_specs=[hbm] * 8,
        out_specs=(vmem, vmem),
        scratch_shapes=[
            pltpu.VMEM((blocks * tok_rows, width), bf16),
            pltpu.VMEM((blocks * lat_rows, width), bf16),
            pltpu.VMEM((tok_rows, width), bf16),
            pltpu.VMEM((lat_rows, width), bf16),
            pltpu.VMEM((2, 1, width), f32),
            pltpu.VMEM((2, width, 2, half_width), bf16),
            pltpu.VMEM((2, width, 2 * half_width), bf16),
            pltpu.VMEM((2, 2 * half_width, width), bf16),
            pltpu.VMEM((2, pairs, 2 * span, LANES), bf16),
            pltpu.VMEM((2, pairs, 1, 2 * span), f32),
            pltpu.VMEM((2, pairs, 1, 2 * span), f32),
            pltpu.VMEM((2, half_width, span), f32),
            pltpu.VMEM((2, half_width, span), bf16),
            pltpu.VMEM((2, half_width, span), bf16),
            dma((4, 2, blocks)),
            dma((2, 2, blocks)),
            dma((8,)),
            dma((2,)),
            dma((2,)),
            dma((2,)),
            dma((2,)),
        ],
        compiler_params=pltpu.CompilerParams(
            collective_id=0, has_side_effects=True, vmem_limit_bytes=VMEM_BYTES
        ),
    )(tokens, latents, w_tok, w_lat, o_tok, o_lat, g_tok, g_lat)


def solution(mesh):
    placed = (
        P(("groups", "tok", "lat"), None),
        P(("tok", "lat"), None),
        P(None, None, None, "rep"),
        P(None, None, None, "rep"),
        P(None, "rep", None),
        P(None, "rep", None),
        P(),
        P(),
    )
    sizes = dict(mesh.shape)
    resident = sizes["lat"] == 2 and sizes["rep"] == 2 and 2 <= sizes["tok"] <= 4
    return jax.shard_map(
        gathered_body if resident else body,
        mesh=mesh,
        in_specs=placed,
        out_specs=(P(("groups", "tok", "lat"), None), P(("groups", "tok", "lat"), None)),
        check_vma=False,
    )
```
